32 devices in a mesh: section: 4 (over y, core), dp: 8 (over z, x).
Axes of the slice: x: 2, y: 2, z: 4, core: 2. Of those that a mesh axis runs over, the one named last changes fastest.
Arguments:
- inputs: bfloat16 [1536, 4096], P('dp'), may hold values from -6 to 6
- output_cotangent: bfloat16 [1536, 4096], P('dp'), may hold values from -6 to 6
- lengths: int32 [16], P('dp'), may hold values from 24 to 96
- query_examples: int32 [16], replicated, may hold values from 0 to 15
- norm_gain: bfloat16 [4, 4096], P('section'), may hold values from 0.5 to 1.5
- value_weight: bfloat16 [4, 4096, 1024], P('section', 'dp'), may hold values from -0.09375 to 0.09375
- output_weight: bfloat16 [4, 4096, 1024], P('section', 'dp'), may hold values from -0.1875 to 0.1875
- input_projection: bfloat16 [4, 32, 4096], P('section'), may hold values from -0.09375 to 0.09375
- output_projection: bfloat16 [4, 32, 1024], P('section'), may hold values from -0.1875 to 0.1875
- fisher_prior: float32 [4, 1024, 1024], P('section'), as said below
Outputs:
- scores: float32 [16, 16], P('dp')
The draws below stay inside these ranges and needn't reach their ends.
Inputs may be any that keep to these rules, and one draw needn't show every extreme that they name: `fisher_prior`: each block's 1024 x 1024 matrix is symmetric and positive definite.
All inputs are finite; a program needn't handle non-finite values.
Results may differ from the reference program's by a relative error of at most 0.0013.
Values may be sent and summed in bfloat16 or wider, within the bound.
A program may use at most 128 MiB of HBM per device.

```python
import math
import jax
import jax.numpy as jnp
from jax import lax

D = 4096
KV = 1024
RI = 32
RO = 32
LEN = 96
QUERIES = 16
SECTIONS = 4
EXAMPLES = 16
TOKENS = 1536
K = 1024


def draw_fisher_prior(key, part):
    factor_key, diagonal_key = jax.random.split(key, 2)
    factors = jax.random.normal(factor_key, (SECTIONS, K, K), jnp.float32)
    shared = jnp.einsum('sij,skj->sik', factors, factors, precision=lax.Precision.HIGHEST) / K
    spread = jnp.exp(jax.random.uniform(diagonal_key, (SECTIONS, K), jnp.float32, math.log(0.5), math.log(4.0)))
    prior_matrix = shared + spread[:, :, None] * jnp.eye(K, dtype=jnp.float32)[None]
    return prior_matrix


def plant(entries, rng, low, high):
    index_at = [jax.random.randint(jax.random.fold_in(rng, axis), (), 0, length) for axis, length in enumerate(entries.shape)]
    longest = entries.shape.index(max(entries.shape))
    beside = index_at[:longest] + [(index_at[longest] + 1) % entries.shape[longest]] + index_at[longest + 1:]
    return entries.at[tuple(index_at)].set(low).at[tuple(beside)].set(high)


def shard_levels(stream_key, shape, cuts, least, largest):
    level, own = 1.0, jax.random.fold_in(stream_key, 6)
    for axis_at, shards_of in cuts:
        draws = jnp.exp(jax.random.uniform(jax.random.fold_in(own, axis_at), (shards_of,), jnp.float32, least / len(cuts), largest / len(cuts)))
        level = level * jnp.repeat(draws, shape[axis_at] // shards_of).reshape([-1 if axis == axis_at else 1 for axis in range(len(shape))])
    return level


def centred(rng, shape, width, most, pieces=(), kind=jnp.bfloat16):
    entries = jax.random.normal(rng, shape, jnp.float32) * width
    if len(pieces) > 0:
        entries = shard_levels(rng, shape, pieces, -0.22, 0.18) * entries
    return jnp.clip(entries, min=-most, max=most).astype(kind)


def setup_inputs(seed: int = 0) -> dict:
    splits = jax.random.split(jax.random.key(seed), 11)
    inputs = centred(splits[0], (TOKENS, D), 1.0, 6.0, ((0, 8),))
    output_cotangent = centred(splits[1], (TOKENS, D), 1.0, 6.0, ((0, 8),))
    lengths = plant(jax.random.randint(splits[2], (EXAMPLES,), LEN // 4, LEN + 1), jax.random.fold_in(splits[2], 1), LEN // 4, LEN).astype(jnp.int32)
    query_examples = plant(jax.random.randint(splits[3], (QUERIES,), 0, EXAMPLES), jax.random.fold_in(splits[3], 1), 0, EXAMPLES - 1).astype(jnp.int32)
    norm_gain = jnp.clip(1.0 + 0.1 * jax.random.normal(splits[4], (SECTIONS, D), jnp.float32), 0.5, 1.5).astype(jnp.bfloat16)
    value_weight = centred(splits[5], (SECTIONS, D, KV), D ** -0.5, 0.09375, ((0, 4), (1, 8)))
    output_weight = centred(splits[6], (SECTIONS, D, KV), KV ** -0.5, 0.1875, ((0, 4), (1, 8)))
    input_projection = centred(splits[7], (SECTIONS, RI, D), D ** -0.5, 0.09375, ((0, 4),))
    output_projection = centred(splits[8], (SECTIONS, RO, KV), KV ** -0.5, 0.1875, ((0, 4),))
    fisher_prior = draw_fisher_prior(jax.random.fold_in(splits[10], 71), 0)
    return dict(inputs=inputs, output_cotangent=output_cotangent, lengths=lengths, query_examples=query_examples, norm_gain=norm_gain, value_weight=value_weight, output_weight=output_weight, input_projection=input_projection, output_projection=output_projection, fisher_prior=fisher_prior)


def normalize(hidden, gain):
    widened = hidden.astype(jnp.float32)
    factor = lax.rsqrt(lax.optimization_barrier(jnp.mean(widened * widened, axis=-1, keepdims=True)) + 1e-05)
    return (widened * factor * gain.astype(jnp.float32)).astype(jnp.bfloat16)

def forward_block(hidden, gain, value_map, output_map, input_map):
    normed = normalize(hidden, gain)
    values = jnp.dot(normed.astype(jnp.float32), value_map.astype(jnp.float32), preferred_element_type=jnp.float32)
    activated = jax.nn.silu(values).astype(jnp.bfloat16)
    branch = lax.dot_general(activated.astype(jnp.float32), output_map.astype(jnp.float32), (((1,), (1,)), ((), ())), preferred_element_type=jnp.float32)
    following = (hidden.astype(jnp.float32) + branch).astype(jnp.bfloat16)
    features = lax.dot_general(normed.astype(jnp.float32), input_map.astype(jnp.float32), (((1,), (1,)), ((), ())), preferred_element_type=jnp.float32).astype(jnp.bfloat16)
    return (following, values, features)

def backward_block(hidden, values, cotangent, gain, value_map, output_map, output_map_small):
    widened = hidden.astype(jnp.float32)
    factor = lax.rsqrt(lax.optimization_barrier(jnp.mean(widened * widened, axis=-1, keepdims=True)) + 1e-05)
    upstream = jnp.dot(cotangent.astype(jnp.float32), output_map.astype(jnp.float32), preferred_element_type=jnp.float32)
    logistic = jax.nn.sigmoid(values)
    slopes = (upstream * logistic * (1.0 + values * (1.0 - logistic))).astype(jnp.bfloat16)
    signals = lax.dot_general(slopes.astype(jnp.float32), output_map_small.astype(jnp.float32), (((1,), (1,)), ((), ())), preferred_element_type=jnp.float32).astype(jnp.bfloat16)
    normed_grad = lax.dot_general(slopes.astype(jnp.float32), value_map.astype(jnp.float32), (((1,), (1,)), ((), ())), preferred_element_type=jnp.float32)
    weighted = normed_grad * gain.astype(jnp.float32)
    inner_mean = lax.optimization_barrier(jnp.mean(weighted * widened, axis=-1, keepdims=True))
    hidden_grad = factor * weighted - widened * (factor * factor * factor) * inner_mean
    previous = (cotangent.astype(jnp.float32) + hidden_grad).astype(jnp.bfloat16)
    return (previous, signals)

def reference(inputs, output_cotangent, lengths, query_examples, norm_gain, value_weight, output_weight, input_projection, output_projection, fisher_prior):
    positions = jnp.arange(LEN, dtype=jnp.int32)
    keep = (positions[None, :] < lengths[:, None]).astype(jnp.bfloat16)
    hidden = inputs
    stored_hidden = []
    stored_values = []
    stored_features = []
    for section in range(SECTIONS):
        stored_hidden.append(hidden)
        hidden, values, features = forward_block(hidden, norm_gain[section], value_weight[section], output_weight[section], input_projection[section])
        stored_values.append(values)
        stored_features.append(features)
    cotangent = (output_cotangent.reshape(EXAMPLES, LEN, D) * keep[:, :, None]).reshape(TOKENS, D)
    scores = jnp.zeros((EXAMPLES, QUERIES), jnp.float32)
    for section in reversed(range(SECTIONS)):
        cotangent, signals = backward_block(stored_hidden[section], stored_values[section], cotangent, norm_gain[section], value_weight[section], output_weight[section], output_projection[section])
        grads = jnp.einsum('elo,eli->eoi', signals.reshape(EXAMPLES, LEN, RO).astype(jnp.float32), stored_features[section].reshape(EXAMPLES, LEN, RI).astype(jnp.float32), precision=lax.Precision.HIGHEST) / LEN
        flat = grads.reshape(EXAMPLES, K)
        fisher = jnp.dot(flat.T, flat, precision=lax.Precision.HIGHEST)
        hessian = fisher_prior[section] + fisher
        chosen = flat[query_examples]
        lower_factor = jnp.linalg.cholesky(hessian)
        solved = jax.scipy.linalg.cho_solve((lower_factor, True), chosen.T)
        scores = scores + jnp.dot(flat, solved, precision=lax.Precision.HIGHEST)
    return scores
```

```python
import jax
import jax.numpy as jnp
from jax import lax
from jax.experimental import pallas as pl
from jax.experimental.pallas import tpu as pltpu
from jax.sharding import PartitionSpec as P


HIGHEST = lax.Precision.HIGHEST


def inverted(block):
    size = block.shape[0]
    rows = lax.broadcasted_iota(jnp.int32, block.shape, 0)
    columns = lax.broadcasted_iota(jnp.int32, block.shape, 1)

    def sweep(pivot, held):
        at_row, at_column = rows == pivot, columns == pivot
        row = jnp.sum(jnp.where(at_row, held, 0.0), axis=0, keepdims=True)
        column = jnp.sum(jnp.where(at_column, held, 0.0), axis=1, keepdims=True)
        corner = jnp.sum(jnp.where(at_column[:1], row, 0.0), axis=1, keepdims=True)
        scale = 1.0 / corner
        scaled = row * scale
        updated = held - column * scaled
        updated = jnp.where(at_row, scaled, updated)
        updated = jnp.where(at_column, column * scale, updated)
        return jnp.where(at_row & at_column, -scale, updated)

    return -lax.fori_loop(0, size, sweep, block)


def invert_in_place(work, strip, block):
    size = work.shape[0]
    count = size // block

    def eliminate(step, carry):
        span = pl.ds(pl.multiple_of(step * block, block), block)
        corner = inverted(work[span, span])
        strip[...] = jnp.dot(
            corner, work[span, :], precision=HIGHEST, preferred_element_type=jnp.float32
        )

        def update(other, carry):
            across = pl.ds(pl.multiple_of(other * block, block), block)
            lead = work[span, across].T

            @pl.when(other != step)
            def _():
                work[across, :] -= jnp.dot(
                    lead, strip[...], precision=HIGHEST, preferred_element_type=jnp.float32
                )
                work[across, span] = strip[:, across].T

            return carry

        lax.fori_loop(0, count, update, 0)
        work[span, :] = strip[...]
        work[span, span] = -corner
        return carry

    lax.fori_loop(0, count, eliminate, 0)


def prior_kernel(prior, work, strip):
    work[...] = prior[...]
    invert_in_place(work, strip, strip.shape[0])


def prior_inverse(prior):
    size = prior.shape[0]
    block = 128
    return pl.pallas_call(
        prior_kernel,
        out_shape=jax.ShapeDtypeStruct((size, size), jnp.float32),
        in_specs=[pl.BlockSpec(memory_space=pltpu.VMEM)],
        out_specs=pl.BlockSpec(memory_space=pltpu.VMEM),
        scratch_shapes=[pltpu.VMEM((block, size), jnp.float32)],
        compiler_params=pltpu.CompilerParams(vmem_limit_bytes=24 * 2**20),
        cost_estimate=pl.CostEstimate(flops=10**11, bytes_accessed=8 * size * size, transcendentals=0),
        name="prior_inverse",
    )(prior)


def score_kernel(everyone, negated, queries, out):
    grads = everyone[...]
    half = jnp.dot(grads, negated[...], precision=HIGHEST, preferred_element_type=jnp.float32)
    gram = -lax.dot_general(
        half, grads, (((1,), (1,)), ((), ())), precision=HIGHEST,
        preferred_element_type=jnp.float32,
    )
    count = grads.shape[0]
    rows = lax.broadcasted_iota(jnp.int32, (count, count), 0)
    columns = lax.broadcasted_iota(jnp.int32, (count, count), 1)
    inverse = inverted(gram + jnp.where(rows == columns, 1.0, 0.0))
    full = jnp.dot(gram, inverse, precision=HIGHEST, preferred_element_type=jnp.float32)
    owners = lax.broadcasted_iota(jnp.int32, (count, queries.shape[1]), 0)
    selector = jnp.where(owners == queries[...], 1.0, 0.0)
    out[...] = jnp.dot(full, selector, precision=HIGHEST, preferred_element_type=jnp.float32)


def all_scores(everyone, negated, queries):
    return pl.pallas_call(
        score_kernel,
        out_shape=jax.ShapeDtypeStruct((everyone.shape[0], queries.shape[0]), jnp.float32),
        in_specs=[pl.BlockSpec(memory_space=pltpu.VMEM)] * 3,
        out_specs=pl.BlockSpec(memory_space=pltpu.VMEM),
        compiler_params=pltpu.CompilerParams(vmem_limit_bytes=24 * 2**20),
        name="all_scores",
    )(everyone, negated, queries[None, :])


def shifted(value, axis, steps):
    count = lax.axis_size(axis)
    first, last = (max(0, -steps), min(count, count - steps))
    return lax.ppermute(value, axis, [(source, source + steps) for source in range(first, last)])


def normalize(hidden, gain):
    widened = hidden.astype(jnp.float32)
    factor = lax.rsqrt(jnp.mean(widened * widened, axis=-1, keepdims=True) + 1e-05)
    return (widened * factor * gain.astype(jnp.float32)).astype(jnp.bfloat16)


def forward_block(hidden, gain, value_map, output_map, input_map):
    normed = normalize(hidden, gain)
    values = jnp.dot(normed, value_map, preferred_element_type=jnp.float32)
    activated = jax.nn.silu(values).astype(jnp.bfloat16)
    branch = lax.dot_general(
        activated, output_map, (((1,), (1,)), ((), ())), preferred_element_type=jnp.float32
    )
    following = (hidden.astype(jnp.float32) + branch).astype(jnp.bfloat16)
    features = lax.dot_general(
        normed, input_map, (((1,), (1,)), ((), ())), preferred_element_type=jnp.float32
    ).astype(jnp.bfloat16)
    return (following, values, features)


def backward_block(hidden, values, cotangent, gain, value_map, output_map, output_map_small):
    widened = hidden.astype(jnp.float32)
    factor = lax.rsqrt(jnp.mean(widened * widened, axis=-1, keepdims=True) + 1e-05)
    upstream = jnp.dot(cotangent, output_map, preferred_element_type=jnp.float32)
    logistic = jax.nn.sigmoid(values)
    slopes = (upstream * logistic * (1.0 + values * (1.0 - logistic))).astype(jnp.bfloat16)
    signals = lax.dot_general(
        slopes, output_map_small, (((1,), (1,)), ((), ())), preferred_element_type=jnp.float32
    ).astype(jnp.bfloat16)
    normed_grad = lax.dot_general(
        slopes, value_map, (((1,), (1,)), ((), ())), preferred_element_type=jnp.float32
    )
    weighted = normed_grad * gain.astype(jnp.float32)
    inner_mean = jnp.mean(weighted * widened, axis=-1, keepdims=True)
    hidden_grad = factor * weighted - widened * (factor * factor * factor) * inner_mean
    previous = (cotangent.astype(jnp.float32) + hidden_grad).astype(jnp.bfloat16)
    return (previous, signals)


def per_device(
    inputs,
    output_cotangent,
    lengths,
    query_examples,
    norm_gain,
    value_weight,
    output_weight,
    input_projection,
    output_projection,
    fisher_prior,
):
    sections = lax.axis_size("section")
    section_index = lax.axis_index("section")
    value_map, output_map = (
        lax.all_gather(value_weight, "dp", axis=1, tiled=True),
        lax.all_gather(output_weight, "dp", axis=1, tiled=True),
    )
    value_map = value_map[0]
    output_map = output_map[0]
    gain = norm_gain[0]
    input_map = input_projection[0]
    output_map_small = output_projection[0]
    negated_inverse = prior_inverse(fisher_prior[0])
    batches = lengths.shape[0]
    example_rows = inputs.shape[0] // batches
    width = inputs.shape[1]
    value_width = value_map.shape[1]
    feature_width = input_map.shape[0]
    signal_width = output_map_small.shape[0]
    entries = inputs.reshape(batches, example_rows, width)
    positions = jnp.arange(example_rows, dtype=jnp.int32)
    keep = (positions[None, :] < lengths[:, None]).astype(jnp.bfloat16)
    targets = output_cotangent.reshape(batches, example_rows, width) * keep[:, :, None]
    ticks = batches + sections - 1

    def forward_running(hidden):
        return forward_block(hidden, gain, value_map, output_map, input_map)

    def forward_skipped(hidden):
        return (
            jnp.zeros_like(hidden),
            jnp.zeros((example_rows, value_width), jnp.float32),
            jnp.zeros((example_rows, feature_width), jnp.bfloat16),
        )

    def forward_tick(tick, carry):
        incoming, saved_hidden, saved_values, saved_features = carry
        turn = tick - section_index
        active = (turn >= 0) & (turn < batches)
        picked = jnp.clip(turn, 0, batches - 1)
        entering = lax.dynamic_index_in_dim(entries, picked, 0, keepdims=False)
        hidden = jnp.where(section_index == 0, entering, incoming)
        following, values, features = lax.cond(active, forward_running, forward_skipped, hidden)
        saved_hidden = jnp.where(
            active, lax.dynamic_update_index_in_dim(saved_hidden, hidden, picked, 0), saved_hidden
        )
        saved_values = jnp.where(
            active, lax.dynamic_update_index_in_dim(saved_values, values, picked, 0), saved_values
        )
        saved_features = jnp.where(
            active,
            lax.dynamic_update_index_in_dim(saved_features, features, picked, 0),
            saved_features,
        )
        incoming = shifted(following, "section", 1)
        return (incoming, saved_hidden, saved_values, saved_features)

    forward_start = (
        jnp.zeros((example_rows, width), jnp.bfloat16),
        jnp.zeros((batches, example_rows, width), jnp.bfloat16),
        jnp.zeros((batches, example_rows, value_width), jnp.float32),
        jnp.zeros((batches, example_rows, feature_width), jnp.bfloat16),
    )
    forward_state = lax.fori_loop(0, ticks, forward_tick, forward_start)
    saved_hidden = forward_state[1]
    saved_values = forward_state[2]
    saved_features = forward_state[3]

    def backward_running(operands):
        hidden, values, cotangent, features = operands
        previous, signals = backward_block(
            hidden, values, cotangent, gain, value_map, output_map, output_map_small
        )
        grads = (
            lax.dot_general(
                signals, features, (((0,), (0,)), ((), ())), preferred_element_type=jnp.float32
            )
            / example_rows
        )
        return (previous, grads)

    def backward_skipped(operands):
        return (
            jnp.zeros((example_rows, width), jnp.bfloat16),
            jnp.zeros((signal_width, feature_width), jnp.float32),
        )

    def backward_tick(tick, carry):
        incoming, saved_grads = carry
        turn = tick - (sections - 1 - section_index)
        active = (turn >= 0) & (turn < batches)
        picked = jnp.clip(turn, 0, batches - 1)
        arriving = lax.dynamic_index_in_dim(targets, picked, 0, keepdims=False)
        cotangent = jnp.where(section_index == sections - 1, arriving, incoming)
        hidden = lax.dynamic_index_in_dim(saved_hidden, picked, 0, keepdims=False)
        values = lax.dynamic_index_in_dim(saved_values, picked, 0, keepdims=False)
        features = lax.dynamic_index_in_dim(saved_features, picked, 0, keepdims=False)
        previous, grads = lax.cond(
            active, backward_running, backward_skipped, (hidden, values, cotangent, features)
        )
        saved_grads = jnp.where(
            active, lax.dynamic_update_index_in_dim(saved_grads, grads, picked, 0), saved_grads
        )
        incoming = shifted(previous, "section", -1)
        return (incoming, saved_grads)

    backward_start = (
        jnp.zeros((example_rows, width), jnp.bfloat16),
        jnp.zeros((batches, signal_width, feature_width), jnp.float32),
    )
    backward_state = lax.fori_loop(0, ticks, backward_tick, backward_start)
    flat = backward_state[1].reshape(batches, signal_width * feature_width)
    everyone = lax.all_gather(flat, "dp", axis=0, tiled=True)
    every_score = all_scores(everyone, negated_inverse, query_examples)
    section_scores = lax.dynamic_slice_in_dim(
        every_score, lax.axis_index("dp") * batches, batches, 0
    )
    return lax.psum(section_scores, "section")


def solution(mesh):
    placed = (
        P("dp", None),
        P("dp", None),
        P("dp"),
        P(),
        P("section", None),
        P("section", "dp", None),
        P("section", "dp", None),
        P("section", None, None),
        P("section", None, None),
        P("section", None, None),
    )
    return jax.shard_map(
        per_device, mesh=mesh, in_specs=placed, out_specs=P("dp", None), check_vma=False
    )
```

```python
import functools

import jax
import jax.numpy as jnp
from jax import lax
from jax.experimental import pallas as pl
from jax.experimental.pallas import tpu as pltpu
from jax.sharding import PartitionSpec as P


HIGHEST = lax.Precision.HIGHEST


def inverted(block):
    size = block.shape[0]
    rows = lax.broadcasted_iota(jnp.int32, block.shape, 0)
    columns = lax.broadcasted_iota(jnp.int32, block.shape, 1)

    def sweep(pivot, held):
        at_row, at_column = rows == pivot, columns == pivot
        row = jnp.sum(jnp.where(at_row, held, 0.0), axis=0, keepdims=True)
        column = jnp.sum(jnp.where(at_column, held, 0.0), axis=1, keepdims=True)
        corner = jnp.sum(jnp.where(at_column[:1], row, 0.0), axis=1, keepdims=True)
        scale = 1.0 / corner
        scaled = row * scale
        updated = held - column * scaled
        updated = jnp.where(at_row, scaled, updated)
        updated = jnp.where(at_column, column * scale, updated)
        return jnp.where(at_row & at_column, -scale, updated)

    return -lax.fori_loop(0, size, sweep, block)


def invert_in_place(work, strip, block):
    size = work.shape[0]
    count = size // block

    def eliminate(step, carry):
        span = pl.ds(pl.multiple_of(step * block, block), block)
        corner = inverted(work[span, span])
        strip[...] = jnp.dot(
            corner, work[span, :], precision=HIGHEST, preferred_element_type=jnp.float32
        )

        def update(other, carry):
            across = pl.ds(pl.multiple_of(other * block, block), block)
            lead = work[span, across].T

            @pl.when(other != step)
            def _():
                work[across, :] -= jnp.dot(
                    lead, strip[...], precision=HIGHEST, preferred_element_type=jnp.float32
                )
                work[across, span] = strip[:, across].T

            return carry

        lax.fori_loop(0, count, update, 0)
        work[span, :] = strip[...]
        work[span, span] = -corner
        return carry

    lax.fori_loop(0, count, eliminate, 0)


def prior_kernel(prior, work, strip):
    work[...] = prior[...]
    invert_in_place(work, strip, strip.shape[0])


def prior_inverse(prior):
    size = prior.shape[0]
    block = 128
    return pl.pallas_call(
        prior_kernel,
        out_shape=jax.ShapeDtypeStruct((size, size), jnp.float32),
        in_specs=[pl.BlockSpec(memory_space=pltpu.VMEM)],
        out_specs=pl.BlockSpec(memory_space=pltpu.VMEM),
        scratch_shapes=[pltpu.VMEM((block, size), jnp.float32)],
        compiler_params=pltpu.CompilerParams(vmem_limit_bytes=24 * 2**20),
        cost_estimate=pl.CostEstimate(flops=10**11, bytes_accessed=8 * size * size, transcendentals=0),
        name="prior_inverse",
    )(prior)


def score_kernel(everyone, negated, queries, out):
    grads = everyone[...]
    half = jnp.dot(grads, negated[...], precision=HIGHEST, preferred_element_type=jnp.float32)
    gram = -lax.dot_general(
        half, grads, (((1,), (1,)), ((), ())), precision=HIGHEST,
        preferred_element_type=jnp.float32,
    )
    count = grads.shape[0]
    rows = lax.broadcasted_iota(jnp.int32, (count, count), 0)
    columns = lax.broadcasted_iota(jnp.int32, (count, count), 1)
    inverse = inverted(gram + jnp.where(rows == columns, 1.0, 0.0))
    full = jnp.dot(gram, inverse, precision=HIGHEST, preferred_element_type=jnp.float32)
    owners = lax.broadcasted_iota(jnp.int32, (count, queries.shape[1]), 0)
    selector = jnp.where(owners == queries[...], 1.0, 0.0)
    out[...] = jnp.dot(full, selector, precision=HIGHEST, preferred_element_type=jnp.float32)


def all_scores(everyone, negated, queries):
    return pl.pallas_call(
        score_kernel,
        out_shape=jax.ShapeDtypeStruct((everyone.shape[0], queries.shape[0]), jnp.float32),
        in_specs=[pl.BlockSpec(memory_space=pltpu.VMEM)] * 3,
        out_specs=pl.BlockSpec(memory_space=pltpu.VMEM),
        compiler_params=pltpu.CompilerParams(vmem_limit_bytes=24 * 2**20),
        name="all_scores",
    )(everyone, negated, queries[None, :])


MESH = pl.DeviceIdType.MESH
CONTRACT_LAST = (((1,), (1,)), ((), ()))


def relay_kernel(
    sections, batches, example_rows,
    inputs, targets, gain, value_map, output_map, input_map, output_map_small,
    grads,
    hidden, following, cotangent, previous, values, normed, activated, features, factors,
    forward_send, forward_receive, backward_send, backward_receive,
):
    me = lax.axis_index("section")
    has_before, has_after = me > 0, me < sections - 1
    before, after = lax.max(me - 1, 0), lax.min(me + 1, sections - 1)
    width, value_width = value_map.shape
    signal_width = output_map_small.shape[0]
    chunks = forward_send.shape[1]
    chunk = width // chunks
    tile = 256
    group = 16

    def span(index, size):
        return pl.ds(pl.multiple_of(index * size, size), size)

    def forward_copy(batch, piece):
        columns = span(piece, chunk)
        return pltpu.make_async_remote_copy(
            src_ref=following.at[batch, :, columns],
            dst_ref=hidden.at[batch, :, columns],
            send_sem=forward_send.at[batch, piece],
            recv_sem=forward_receive.at[batch, piece],
            device_id={"section": after},
            device_id_type=MESH,
        )

    def backward_copy(batch, piece):
        columns = span(piece, chunk)
        return pltpu.make_async_remote_copy(
            src_ref=previous.at[batch, :, columns],
            dst_ref=cotangent.at[batch, :, columns],
            send_sem=backward_send.at[batch, piece],
            recv_sem=backward_receive.at[batch, piece],
            device_id={"section": before},
            device_id_type=MESH,
        )

    barrier = pltpu.get_barrier_semaphore()

    @pl.when(has_before)
    def _():
        pl.semaphore_signal(barrier, inc=1, device_id={"section": before}, device_id_type=MESH)

    @pl.when(has_after)
    def _():
        pl.semaphore_signal(barrier, inc=1, device_id={"section": after}, device_id_type=MESH)

    peers = lax.min(me, 1) + lax.min(sections - 1 - me, 1)
    pl.semaphore_wait(barrier, peers)

    @pl.loop(0, batches)
    def _(batch):
        @pl.when(has_before)
        def _():
            @pl.loop(0, chunks)
            def _(piece):
                forward_copy(batch, piece).wait_recv()

        @pl.when(jnp.logical_not(has_before))
        def _():
            hidden[batch] = inputs[batch]

        @pl.loop(0, example_rows // group)
        def _(at):
            rows = span(at, group)
            widened = hidden[batch, rows, :].astype(jnp.float32)
            factor = lax.rsqrt(jnp.mean(widened * widened, axis=-1, keepdims=True) + 1e-05)
            factors[batch, rows, :] = factor
            normed[rows, :] = (widened * factor * gain[...]).astype(jnp.bfloat16)

        @pl.loop(0, value_width // tile)
        def _(at):
            columns = span(at, tile)
            found = jnp.dot(
                normed[...], value_map[:, columns], preferred_element_type=jnp.float32
            )
            values[batch, :, columns] = found
            activated[:, columns] = (found / (1.0 + jnp.exp(-found))).astype(jnp.bfloat16)

        @pl.when(has_after)
        def _():
            @pl.loop(0, chunks)
            def _(piece):
                columns = span(piece, chunk)
                branch = lax.dot_general(
                    activated[...], output_map[columns, :], CONTRACT_LAST,
                    preferred_element_type=jnp.float32,
                )
                following[batch, :, columns] = (
                    hidden[batch, :, columns].astype(jnp.float32) + branch
                ).astype(jnp.bfloat16)
                forward_copy(batch, piece).start()

        features[batch] = lax.dot_general(
            normed[...], input_map[...], CONTRACT_LAST, preferred_element_type=jnp.float32
        ).astype(jnp.bfloat16)

    @pl.loop(0, batches)
    def _(batch):
        @pl.when(has_after)
        def _():
            @pl.loop(0, chunks)
            def _(piece):
                backward_copy(batch, piece).wait_recv()

        @pl.when(jnp.logical_not(has_after))
        def _():
            cotangent[batch] = targets[batch]

        slopes = activated

        def upstream_tile(at, total):
            columns = span(at, tile)
            upstream = jnp.dot(
                cotangent[batch], output_map[:, columns], preferred_element_type=jnp.float32
            )
            found = values[batch, :, columns]
            logistic = 1.0 / (1.0 + jnp.exp(-found))
            slope = (upstream * logistic * (1.0 + found * (1.0 - logistic))).astype(jnp.bfloat16)
            slopes[:, columns] = slope
            return total + jnp.sum(slope.astype(jnp.float32) * found, axis=-1, keepdims=True)

        total = lax.fori_loop(
            0, value_width // tile, upstream_tile, jnp.zeros((example_rows, 1), jnp.float32)
        )
        factor = factors[batch]
        shrink = total * (factor * factor) * (1.0 / width)

        @pl.when(has_before)
        def _():
            @pl.loop(0, chunks)
            def _(piece):
                columns = span(piece, chunk)
                normed_grad = lax.dot_general(
                    slopes[...], value_map[columns, :], CONTRACT_LAST,
                    preferred_element_type=jnp.float32,
                )
                weighted = normed_grad * gain[:, columns]
                hidden_grad = (
                    factor * weighted - hidden[batch, :, columns].astype(jnp.float32) * shrink
                )
                previous[batch, :, columns] = (
                    cotangent[batch, :, columns].astype(jnp.float32) + hidden_grad
                ).astype(jnp.bfloat16)
                backward_copy(batch, piece).start()

        signals = lax.dot_general(
            slopes[...], output_map_small[...], CONTRACT_LAST, preferred_element_type=jnp.float32
        ).astype(jnp.bfloat16)
        grads[batch] = lax.dot_general(
            signals, features[batch], (((0,), (0,)), ((), ())), preferred_element_type=jnp.float32
        ) * (1.0 / example_rows)

    @pl.loop(0, batches)
    def _(batch):
        @pl.loop(0, chunks)
        def _(piece):
            @pl.when(has_after)
            def _():
                forward_copy(batch, piece).wait_send()

            @pl.when(has_before)
            def _():
                backward_copy(batch, piece).wait_send()


def relay(inputs, targets, gain, value_map, output_map, input_map, output_map_small):
    batches, example_rows, width = inputs.shape
    value_width = value_map.shape[1]
    feature_width = input_map.shape[0]
    signal_width = output_map_small.shape[0]
    chunks = 8
    stream = pltpu.VMEM((batches, example_rows, width), jnp.bfloat16)
    return pl.pallas_call(
        functools.partial(relay_kernel, lax.axis_size("section"), batches, example_rows),
        out_shape=jax.ShapeDtypeStruct((batches, signal_width, feature_width), jnp.float32),
        in_specs=[pl.BlockSpec(memory_space=pltpu.VMEM)] * 7,
        out_specs=pl.BlockSpec(memory_space=pltpu.VMEM),
        scratch_shapes=[
            stream, stream, stream, stream,
            pltpu.VMEM((batches, example_rows, value_width), jnp.float32),
            pltpu.VMEM((example_rows, width), jnp.bfloat16),
            pltpu.VMEM((example_rows, value_width), jnp.bfloat16),
            pltpu.VMEM((batches, example_rows, feature_width), jnp.bfloat16),
            pltpu.VMEM((batches, example_rows, 1), jnp.float32),
        ] + [pltpu.SemaphoreType.DMA((batches, chunks))] * 4,
        compiler_params=pltpu.CompilerParams(
            collective_id=1, has_side_effects=True, vmem_limit_bytes=48 * 2**20
        ),
        name="relay",
    )(inputs, targets, gain, value_map, output_map, input_map, output_map_small)


def per_device(
    inputs,
    output_cotangent,
    lengths,
    query_examples,
    norm_gain,
    value_weight,
    output_weight,
    input_projection,
    output_projection,
    fisher_prior,
):
    value_map, output_map = (
        lax.all_gather(value_weight, "dp", axis=1, tiled=True),
        lax.all_gather(output_weight, "dp", axis=1, tiled=True),
    )
    value_map = value_map[0]
    output_map = output_map[0]
    gain = norm_gain.astype(jnp.float32)
    input_map = input_projection[0]
    output_map_small = output_projection[0]
    negated_inverse = prior_inverse(fisher_prior[0])
    batches = lengths.shape[0]
    example_rows = inputs.shape[0] // batches
    width = inputs.shape[1]
    feature_width = input_map.shape[0]
    signal_width = output_map_small.shape[0]
    entries = inputs.reshape(batches, example_rows, width)
    positions = jnp.arange(example_rows, dtype=jnp.int32)
    keep = (positions[None, :] < lengths[:, None]).astype(jnp.bfloat16)
    targets = output_cotangent.reshape(batches, example_rows, width) * keep[:, :, None]
    saved_grads = relay(
        entries, targets, gain, value_map, output_map, input_map, output_map_small
    )
    flat = saved_grads.reshape(batches, signal_width * feature_width)
    everyone = lax.all_gather(flat, "dp", axis=0, tiled=True)
    every_score = all_scores(everyone, negated_inverse, query_examples)
    section_scores = lax.dynamic_slice_in_dim(
        every_score, lax.axis_index("dp") * batches, batches, 0
    )
    return lax.psum(section_scores, "section")


def solution(mesh):
    placed = (
        P("dp", None),
        P("dp", None),
        P("dp"),
        P(),
        P("section", None),
        P("section", "dp", None),
        P("section", "dp", None),
        P("section", None, None),
        P("section", None, None),
        P("section", None, None),
    )
    return jax.shard_map(
        per_device, mesh=mesh, in_specs=placed, out_specs=P("dp", None), check_vma=False
    )
```

```python
import functools

import jax
import jax.numpy as jnp
from jax import lax
from jax.experimental import pallas as pl
from jax.experimental.pallas import tpu as pltpu
from jax.sharding import PartitionSpec as P


HIGHEST = lax.Precision.HIGHEST


def inverted(block):
    size = block.shape[0]
    rows = lax.broadcasted_iota(jnp.int32, block.shape, 0)
    columns = lax.broadcasted_iota(jnp.int32, block.shape, 1)

    def sweep(pivot, held):
        at_row, at_column = rows == pivot, columns == pivot
        row = jnp.sum(jnp.where(at_row, held, 0.0), axis=0, keepdims=True)
        column = jnp.sum(jnp.where(at_column, held, 0.0), axis=1, keepdims=True)
        corner = jnp.sum(jnp.where(at_column[:1], row, 0.0), axis=1, keepdims=True)
        scale = 1.0 / corner
        scaled = row * scale
        updated = held - column * scaled
        updated = jnp.where(at_row, scaled, updated)
        updated = jnp.where(at_column, column * scale, updated)
        return jnp.where(at_row & at_column, -scale, updated)

    return -lax.fori_loop(0, size, sweep, block)


def sweep_strip(work, strip, step, block):
    span = pl.ds(pl.multiple_of(step * block, block), block)
    corner = inverted(work[span, span])
    strip[...] = jnp.dot(
        corner, work[span, :], precision=HIGHEST, preferred_element_type=jnp.float32
    )
    strip[:, span] = -corner


def sweep_rest(work, strip, step, block):
    span = pl.ds(pl.multiple_of(step * block, block), block)

    @pl.loop(0, work.shape[0] // block)
    def _(other):
        across = pl.ds(pl.multiple_of(other * block, block), block)

        @pl.when(other != step)
        def _():
            work[across, :] -= jnp.dot(
                work[span, across].T, strip[...], precision=HIGHEST,
                preferred_element_type=jnp.float32,
            )
            work[across, span] = strip[:, across].T

    work[span, :] = strip[...]


def ring_device(place, count):
    if count % 4 or count < 8:
        return place
    fast = count // 4
    inner = lax.min(place, 1) * lax.min(lax.max(4 * (fast - 1) + 1 - place, 0), 1)
    along = lax.max(place - 1, 0)
    row, step = lax.div(along, fast - 1), lax.rem(along, fast - 1)
    odd = lax.rem(row, 2)
    column = 1 + (1 - odd) * step + odd * (fast - 2 - step)
    return inner * (row * fast + column) + (1 - inner) * lax.rem(count - place, count) * fast


def ring_place(device, count):
    if count % 4 or count < 8:
        return device
    fast = count // 4
    row, column = lax.div(device, fast), lax.rem(device, fast)
    inner = lax.min(column, 1)
    odd = lax.rem(row, 2)
    within = 1 + row * (fast - 1) + (1 - odd) * (column - 1) + odd * (fast - 1 - column)
    return inner * within + (1 - inner) * lax.rem(count - row, count)


def gather_kernel(
    count, value_shard, output_shard, prior, value_all, output_all, work, strip,
    send, receive, own,
):
    me = lax.axis_index("dp")
    place = ring_place(me, count)
    targets = [
        ring_device(lax.rem(place + 1, count), count),
        ring_device(lax.rem(place + count - 1, count), count),
    ]
    shards, wholes = (value_shard, output_shard), (value_all, output_all)
    rows = value_shard.shape[0]
    half = rows // 2

    def piece(way, array, step, first):
        back = count - step if way == 0 else step
        origin = ring_device(lax.rem(place + back, count), count)
        start = pl.multiple_of(origin * rows + way * half, half)
        there = wholes[array].at[pl.ds(start, half), :]
        here = shards[array].at[pl.ds(way * half, half), :] if first else there
        return pltpu.make_async_remote_copy(
            src_ref=here,
            dst_ref=there,
            send_sem=send.at[way, array, step],
            recv_sem=receive.at[way, array, step],
            device_id={"dp": targets[way]},
            device_id_type=pl.DeviceIdType.MESH,
        )

    barrier = pltpu.get_barrier_semaphore()
    for target in targets:
        pl.semaphore_signal(
            barrier, inc=1, device_id={"dp": target}, device_id_type=pl.DeviceIdType.MESH
        )
    pl.semaphore_wait(barrier, 2)
    for array in range(2):
        for way in range(2):
            piece(way, array, 0, True).start()
    mine = pl.ds(pl.multiple_of(me * rows, rows), rows)
    kept = [
        pltpu.make_async_copy(shards[array], wholes[array].at[mine, :], own.at[array])
        for array in range(2)
    ]
    for copy in kept:
        copy.start()
    work[...] = prior[...]
    block = strip.shape[0]
    blocks = work.shape[0] // block

    def pass_on(array, step):
        for way in range(2):
            piece(way, array, step, False).wait_recv()

            @pl.when(step < count - 2)
            def _():
                piece(way, array, lax.min(step + 1, count - 2), False).start()

    @pl.loop(0, max(blocks, count - 1))
    def _(step):
        @pl.when(step < blocks)
        def _():
            sweep_strip(work, strip, step, block)

        @pl.when(step < count - 1)
        def _():
            pass_on(0, step)

        @pl.when(step < blocks)
        def _():
            sweep_rest(work, strip, step, block)

        @pl.when(step < count - 1)
        def _():
            pass_on(1, step)

    for copy in kept:
        copy.wait()
    for array in range(2):
        for way in range(2):
            piece(way, array, 0, True).wait_send()

            @pl.loop(1, count - 1)
            def _(step):
                piece(way, array, step, False).wait_send()


def gathered(value_shard, output_shard, prior):
    count = lax.axis_size("dp")
    rows, columns = value_shard.shape
    size = prior.shape[0]
    whole = jax.ShapeDtypeStruct((count * rows, columns), jnp.bfloat16)
    return pl.pallas_call(
        functools.partial(gather_kernel, count),
        out_shape=(whole, whole, jax.ShapeDtypeStruct((size, size), jnp.float32)),
        in_specs=[pl.BlockSpec(memory_space=pltpu.VMEM)] * 3,
        out_specs=(
            pl.BlockSpec(memory_space=pl.ANY),
            pl.BlockSpec(memory_space=pl.ANY),
            pl.BlockSpec(memory_space=pltpu.VMEM),
        ),
        scratch_shapes=[
            pltpu.VMEM((128, size), jnp.float32),
            pltpu.SemaphoreType.DMA((2, 2, count - 1)),
            pltpu.SemaphoreType.DMA((2, 2, count - 1)),
            pltpu.SemaphoreType.DMA((2,)),
        ],
        compiler_params=pltpu.CompilerParams(
            collective_id=2, has_side_effects=True, vmem_limit_bytes=48 * 2**20
        ),
        name="gather_and_invert",
    )(value_shard, output_shard, prior)


def score_kernel(everyone, negated, queries, out):
    grads = everyone[...]
    half = jnp.dot(grads, negated[...], precision=HIGHEST, preferred_element_type=jnp.float32)
    gram = -lax.dot_general(
        half, grads, (((1,), (1,)), ((), ())), precision=HIGHEST,
        preferred_element_type=jnp.float32,
    )
    count = grads.shape[0]
    rows = lax.broadcasted_iota(jnp.int32, (count, count), 0)
    columns = lax.broadcasted_iota(jnp.int32, (count, count), 1)
    inverse = inverted(gram + jnp.where(rows == columns, 1.0, 0.0))
    full = jnp.dot(gram, inverse, precision=HIGHEST, preferred_element_type=jnp.float32)
    owners = lax.broadcasted_iota(jnp.int32, (count, queries.shape[1]), 0)
    selector = jnp.where(owners == queries[...], 1.0, 0.0)
    out[...] = jnp.dot(full, selector, precision=HIGHEST, preferred_element_type=jnp.float32)


def all_scores(everyone, negated, queries):
    return pl.pallas_call(
        score_kernel,
        out_shape=jax.ShapeDtypeStruct((everyone.shape[0], queries.shape[0]), jnp.float32),
        in_specs=[pl.BlockSpec(memory_space=pltpu.VMEM)] * 3,
        out_specs=pl.BlockSpec(memory_space=pltpu.VMEM),
        compiler_params=pltpu.CompilerParams(vmem_limit_bytes=24 * 2**20),
        name="all_scores",
    )(everyone, negated, queries[None, :])


MESH = pl.DeviceIdType.MESH
CONTRACT_LAST = (((1,), (1,)), ((), ()))


def relay_kernel(
    sections, batches, example_rows,
    inputs, targets, gain, value_map, output_map, input_map, output_map_small,
    grads,
    hidden, following, cotangent, previous, values, normed, activated, features, factors,
    forward_send, forward_receive, backward_send, backward_receive,
):
    me = lax.axis_index("section")
    has_before, has_after = me > 0, me < sections - 1
    before, after = lax.max(me - 1, 0), lax.min(me + 1, sections - 1)
    width, value_width = value_map.shape
    signal_width = output_map_small.shape[0]
    chunks = forward_send.shape[1]
    chunk = width // chunks
    tile = 256
    group = 16

    def span(index, size):
        return pl.ds(pl.multiple_of(index * size, size), size)

    def forward_copy(batch, piece):
        columns = span(piece, chunk)
        return pltpu.make_async_remote_copy(
            src_ref=following.at[batch, :, columns],
            dst_ref=hidden.at[batch, :, columns],
            send_sem=forward_send.at[batch, piece],
            recv_sem=forward_receive.at[batch, piece],
            device_id={"section": after},
            device_id_type=MESH,
        )

    def backward_copy(batch, piece):
        columns = span(piece, chunk)
        return pltpu.make_async_remote_copy(
            src_ref=previous.at[batch, :, columns],
            dst_ref=cotangent.at[batch, :, columns],
            send_sem=backward_send.at[batch, piece],
            recv_sem=backward_receive.at[batch, piece],
            device_id={"section": before},
            device_id_type=MESH,
        )

    barrier = pltpu.get_barrier_semaphore()

    @pl.when(has_before)
    def _():
        pl.semaphore_signal(barrier, inc=1, device_id={"section": before}, device_id_type=MESH)

    @pl.when(has_after)
    def _():
        pl.semaphore_signal(barrier, inc=1, device_id={"section": after}, device_id_type=MESH)

    peers = lax.min(me, 1) + lax.min(sections - 1 - me, 1)
    pl.semaphore_wait(barrier, peers)

    @pl.loop(0, batches)
    def _(batch):
        @pl.when(has_before)
        def _():
            @pl.loop(0, chunks)
            def _(piece):
                forward_copy(batch, piece).wait_recv()

        @pl.when(jnp.logical_not(has_before))
        def _():
            hidden[batch] = inputs[batch]

        @pl.loop(0, example_rows // group)
        def _(at):
            rows = span(at, group)
            widened = hidden[batch, rows, :].astype(jnp.float32)
            factor = lax.rsqrt(jnp.mean(widened * widened, axis=-1, keepdims=True) + 1e-05)
            factors[batch, rows, :] = factor
            normed[rows, :] = (widened * factor * gain[...]).astype(jnp.bfloat16)

        @pl.loop(0, value_width // tile)
        def _(at):
            columns = span(at, tile)
            found = jnp.dot(
                normed[...], value_map[:, columns], preferred_element_type=jnp.float32
            )
            values[batch, :, columns] = found
            activated[:, columns] = (found / (1.0 + jnp.exp(-found))).astype(jnp.bfloat16)

        @pl.when(has_after)
        def _():
            @pl.loop(0, chunks)
            def _(piece):
                columns = span(piece, chunk)
                branch = lax.dot_general(
                    activated[...], output_map[columns, :], CONTRACT_LAST,
                    preferred_element_type=jnp.float32,
                )
                following[batch, :, columns] = (
                    hidden[batch, :, columns].astype(jnp.float32) + branch
                ).astype(jnp.bfloat16)
                forward_copy(batch, piece).start()

        features[batch] = lax.dot_general(
            normed[...], input_map[...], CONTRACT_LAST, preferred_element_type=jnp.float32
        ).astype(jnp.bfloat16)

    @pl.loop(0, batches)
    def _(batch):
        @pl.when(has_after)
        def _():
            @pl.loop(0, chunks)
            def _(piece):
                backward_copy(batch, piece).wait_recv()

        @pl.when(jnp.logical_not(has_after))
        def _():
            cotangent[batch] = targets[batch]

        slopes = activated

        def upstream_tile(at, total):
            columns = span(at, tile)
            upstream = jnp.dot(
                cotangent[batch], output_map[:, columns], preferred_element_type=jnp.float32
            )
            found = values[batch, :, columns]
            logistic = 1.0 / (1.0 + jnp.exp(-found))
            slope = (upstream * logistic * (1.0 + found * (1.0 - logistic))).astype(jnp.bfloat16)
            slopes[:, columns] = slope
            return total + jnp.sum(slope.astype(jnp.float32) * found, axis=-1, keepdims=True)

        total = lax.fori_loop(
            0, value_width // tile, upstream_tile, jnp.zeros((example_rows, 1), jnp.float32)
        )
        factor = factors[batch]
        shrink = total * (factor * factor) * (1.0 / width)

        @pl.when(has_before)
        def _():
            @pl.loop(0, chunks)
            def _(piece):
                columns = span(piece, chunk)
                normed_grad = lax.dot_general(
                    slopes[...], value_map[columns, :], CONTRACT_LAST,
                    preferred_element_type=jnp.float32,
                )
                weighted = normed_grad * gain[:, columns]
                hidden_grad = (
                    factor * weighted - hidden[batch, :, columns].astype(jnp.float32) * shrink
                )
                previous[batch, :, columns] = (
                    cotangent[batch, :, columns].astype(jnp.float32) + hidden_grad
                ).astype(jnp.bfloat16)
                backward_copy(batch, piece).start()

        signals = lax.dot_general(
            slopes[...], output_map_small[...], CONTRACT_LAST, preferred_element_type=jnp.float32
        ).astype(jnp.bfloat16)
        grads[batch] = lax.dot_general(
            signals, features[batch], (((0,), (0,)), ((), ())), preferred_element_type=jnp.float32
        ) * (1.0 / example_rows)

    @pl.loop(0, batches)
    def _(batch):
        @pl.loop(0, chunks)
        def _(piece):
            @pl.when(has_after)
            def _():
                forward_copy(batch, piece).wait_send()

            @pl.when(has_before)
            def _():
                backward_copy(batch, piece).wait_send()


def relay(inputs, targets, gain, value_map, output_map, input_map, output_map_small):
    batches, example_rows, width = inputs.shape
    value_width = value_map.shape[1]
    feature_width = input_map.shape[0]
    signal_width = output_map_small.shape[0]
    chunks = 8
    stream = pltpu.VMEM((batches, example_rows, width), jnp.bfloat16)
    return pl.pallas_call(
        functools.partial(relay_kernel, lax.axis_size("section"), batches, example_rows),
        out_shape=jax.ShapeDtypeStruct((batches, signal_width, feature_width), jnp.float32),
        in_specs=[pl.BlockSpec(memory_space=pltpu.VMEM)] * 7,
        out_specs=pl.BlockSpec(memory_space=pltpu.VMEM),
        scratch_shapes=[
            stream, stream, stream, stream,
            pltpu.VMEM((batches, example_rows, value_width), jnp.float32),
            pltpu.VMEM((example_rows, width), jnp.bfloat16),
            pltpu.VMEM((example_rows, value_width), jnp.bfloat16),
            pltpu.VMEM((batches, example_rows, feature_width), jnp.bfloat16),
            pltpu.VMEM((batches, example_rows, 1), jnp.float32),
        ] + [pltpu.SemaphoreType.DMA((batches, chunks))] * 4,
        compiler_params=pltpu.CompilerParams(
            collective_id=1, has_side_effects=True, vmem_limit_bytes=48 * 2**20
        ),
        name="relay",
    )(inputs, targets, gain, value_map, output_map, input_map, output_map_small)


def per_device(
    inputs,
    output_cotangent,
    lengths,
    query_examples,
    norm_gain,
    value_weight,
    output_weight,
    input_projection,
    output_projection,
    fisher_prior,
):
    value_map, output_map, negated_inverse = gathered(
        value_weight[0], output_weight[0], fisher_prior[0]
    )
    gain = norm_gain.astype(jnp.float32)
    input_map = input_projection[0]
    output_map_small = output_projection[0]
    batches = lengths.shape[0]
    example_rows = inputs.shape[0] // batches
    width = inputs.shape[1]
    feature_width = input_map.shape[0]
    signal_width = output_map_small.shape[0]
    entries = inputs.reshape(batches, example_rows, width)
    positions = jnp.arange(example_rows, dtype=jnp.int32)
    keep = (positions[None, :] < lengths[:, None]).astype(jnp.bfloat16)
    targets = output_cotangent.reshape(batches, example_rows, width) * keep[:, :, None]
    saved_grads = relay(
        entries, targets, gain, value_map, output_map, input_map, output_map_small
    )
    flat = saved_grads.reshape(batches, signal_width * feature_width)
    everyone = lax.all_gather(flat, "dp", axis=0, tiled=True)
    every_score = all_scores(everyone, negated_inverse, query_examples)
    section_scores = lax.dynamic_slice_in_dim(
        every_score, lax.axis_index("dp") * batches, batches, 0
    )
    return lax.psum(section_scores, "section")


def solution(mesh):
    placed = (
        P("dp", None),
        P("dp", None),
        P("dp"),
        P(),
        P("section", None),
        P("section", "dp", None),
        P("section", "dp", None),
        P("section", None, None),
        P("section", None, None),
        P("section", None, None),
    )
    return jax.shard_map(
        per_device, mesh=mesh, in_specs=placed, out_specs=P("dp", None), check_vma=False
    )
```
